32 devices in a mesh: gx: 4 (over z), gy: 4 (over y, x), gz: 2 (over core).
Axes of the slice: x: 2, y: 2, z: 4, core: 2. Of those that a mesh axis runs over, the one named last changes fastest.
Arguments:
- coefficients: bfloat16 [32, 64, 32, 128], P('gx', 'gy', 'gz'), may hold values from -0.109375 to 0.109375
- potential: float32 [32, 64, 32], P('gx', 'gy', 'gz'), may hold values from 0.5 to 2
- owner_map: int32 [4, 4, 2, 7, 1], P('gx', 'gy', 'gz'), may hold values from 0 to 3; in each aligned block of 7 rows (0 to 6, 7 to 13, ..., all dimensions but the last counted through in order) at most 2 rows name the same one
Outputs:
- correction: bfloat16 [4, 4, 2, 8, 128, 128], P('gx', 'gy', 'gz')
The draws below stay inside these ranges and needn't reach their ends.
Inputs may be any that keep to these rules, and one draw needn't show every extreme that they name: `owner_map`: among the 7 blocks of one subdomain no owner is named more than 2 times; in every draw some subdomain names some owner exactly 2 times.
All inputs are finite; a program needn't handle non-finite values.
Results may differ from the reference program's by a relative error of at most 0.0062.
Values may be sent and summed in bfloat16 or wider, within the bound.
No kernel may reach another device: no remote copies, remote signals or barrier semaphores. Data moves between devices by JAX's collectives and lax.ppermute only.
A program may use at most 64 MiB of HBM per device.

```python
import math
import jax
import jax.numpy as jnp
import numpy as np
from jax import lax

NORB = 128
CX = 8
CY = 16
CZ = 16
BLOCKS = 7
CAP = 2
NX = 32
NY = 64
NZ = 32
N_GX = 4
N_GY = 4
N_GZ = 2


def shard_levels(own_key, shape, cuts, low, largest):
    factor_of, own = 1.0, jax.random.fold_in(own_key, 6)
    for dim, blocks in cuts:
        steps = jnp.exp(jax.random.uniform(jax.random.fold_in(own, dim), (blocks,), jnp.float32, low / len(cuts), largest / len(cuts)))
        factor_of = factor_of * jnp.repeat(steps, shape[dim] // blocks).reshape([-1 if axis == dim else 1 for axis in range(len(shape))])
    return factor_of


def assign_block(own_key, own, number, rows, amount, top, limit, lean):
    sequence = jax.random.permutation(own_key, amount)
    crowded, usual = shares(amount, rows * top, limit, lean, True), shares(amount, rows * top, limit, lean, False)
    places = jnp.arange(amount)

    def named(sizes, rotation):
        used = int((sizes > 0).sum())
        fixed = max(1, used // 4)
        moved = fixed + (places - fixed + rotation * (used - fixed)) % max(1, amount - fixed)
        return jnp.zeros((amount,), jnp.int32).at[sequence[jnp.where(places < fixed, places, moved)]].set(jnp.asarray(sizes, jnp.int32))

    sizes = jnp.where(number % 4 == 0, named(crowded, number // 4), named(usual, number - number // 4 - 1))
    mixed = jax.random.permutation(jax.random.fold_in(own, 3), amount)
    donor, taker = mixed[0:amount // 2 * 2:2], mixed[1:amount // 2 * 2:2]
    room = jnp.minimum(sizes[donor] - 1, limit - sizes[taker]) // 2
    room = jnp.where((donor == sequence[0]) | (taker == sequence[0]) | (sizes[taker] == 0), 0, jnp.maximum(room, 0))
    moved = jax.random.randint(jax.random.fold_in(own, 4), (amount // 2,), 0, 1 << 20) % (room + 1)
    sizes = sizes.at[donor].add(-moved).at[taker].add(moved)
    labels = jnp.searchsorted(jnp.cumsum(sizes), jnp.arange(rows * top), side="right").astype(jnp.int32)
    listing = labels.reshape(top, rows).T
    listing = listing[jax.random.permutation(jax.random.fold_in(own, 1), rows)]
    rotation = jax.random.randint(jax.random.fold_in(own, 2), (rows, 1), 0, top)
    return jnp.take_along_axis(listing, (jnp.arange(top)[None, :] + rotation) % top, axis=1)


def shares(count, total, bound, lean, full):
    weights = [(1 << 20) // math.isqrt(rank ** lean) + 1 for rank in range(1, count + 1)]
    largest = bound if full else min(bound, max(-(-total // count), total * weights[0] // sum(weights)))
    least = 1 if total - largest >= count - 1 else 0
    counts, rest = [largest] + [least] * (count - 1), total - largest - least * (count - 1)
    while rest > 0:
        candidates = [i for i in range(1, count) if counts[i] < largest] or [i for i in range(1, count) if counts[i] < bound]
        pool, remaining = sum([weights[i] for i in candidates]), rest
        for i in candidates:
            more = min(bound - counts[i], max(1, remaining * weights[i] // pool), rest)
            counts[i] = counts[i] + more
            rest = rest - more
    return np.array(counts)


def scatter_about(rng, shape, scale, reach, split=(), kind=jnp.bfloat16):
    drawn = jax.random.normal(rng, shape, jnp.float32) * scale
    if len(split) > 0:
        drawn = shard_levels(rng, shape, split, -0.22, 0.18) * drawn
    return jnp.clip(drawn, min=-reach, max=reach).astype(kind)


def setup_inputs(seed: int = 0) -> dict:
    splits = jax.random.split(jax.random.key(seed), 4)
    coefficients = scatter_about(splits[0], (NX, NY, NZ, NORB), (CX * CY * CZ * 1.375) ** -0.5, 0.109375, ((0, 4), (1, 4), (2, 2)))
    potential = jnp.clip(0.5 + 1.5 * jax.random.uniform(splits[1], (NX, NY, NZ), jnp.float32) ** shard_levels(splits[1], (NX, NY, NZ), ((0, 4), (1, 4), (2, 2)), -0.2, 0.2), 0.5, 2.0)
    owner_map_keys = jax.random.split(jax.random.fold_in(splits[2], 1), N_GX * N_GY * N_GZ * BLOCKS // BLOCKS)
    owner_map_turns = jax.random.permutation(jax.random.fold_in(splits[2], 3), N_GX * N_GY * N_GZ * BLOCKS // BLOCKS)
    owner_map = jax.vmap(lambda own, number: assign_block(jax.random.fold_in(splits[2], 2), own, number, BLOCKS, N_GX, 1, CAP, 2))(owner_map_keys, owner_map_turns).reshape((N_GX, N_GY, N_GZ, BLOCKS, 1))
    return dict(coefficients=coefficients, potential=potential, owner_map=owner_map)


SMOOTH = 0.25


def moved(field, dim, step):
    count = field.shape[dim]
    zero = jnp.zeros_like(lax.slice_in_dim(field, 0, 1, axis=dim))
    if step > 0:
        return jnp.concatenate([lax.slice_in_dim(field, 1, count, axis=dim), zero], axis=dim)
    return jnp.concatenate([zero, lax.slice_in_dim(field, 0, count - 1, axis=dim)], axis=dim)


def neighbour_sum(field, dims):
    total = jnp.zeros(field.shape, jnp.float32)
    for dim in dims:
        total = total + moved(field, dim, 1).astype(jnp.float32) + moved(field, dim, -1).astype(jnp.float32)
    return total


def gram(left, right):
    width = left.shape[-1]
    return jnp.dot(left.reshape(-1, width).T, right.reshape(-1, right.shape[-1]), preferred_element_type=jnp.float32)


def one_device(index, coefficients, potential):
    first = (index // (N_GY * N_GZ)).astype(jnp.int32)
    second = ((index // N_GZ) % N_GY).astype(jnp.int32)
    third = (index % N_GZ).astype(jnp.int32)
    cells = (CX, CY, CZ)
    whole = (NX, NY, NZ)
    place = (first, second, third)
    starts = [(first * CX).astype(jnp.int32), (second * CY).astype(jnp.int32), (third * CZ).astype(jnp.int32)]
    zero = jnp.zeros((), jnp.int32)
    block = lax.dynamic_slice(coefficients, (starts[0], starts[1], starts[2], zero), (CX, CY, CZ, NORB))
    local_pot = lax.dynamic_slice(potential, (starts[0], starts[1], starts[2]), (CX, CY, CZ))
    smooth = (block.astype(jnp.float32) + SMOOTH * neighbour_sum(block, (0, 1, 2))).astype(jnp.bfloat16)
    weighted = (local_pot[..., None] * smooth.astype(jnp.float32)).astype(jnp.bfloat16)
    hamilton = gram(smooth, weighted).astype(jnp.bfloat16)
    correlation = gram(smooth, smooth)
    faces = []
    for dim in range(3):
        lateral = tuple(other for other in range(3) if other != dim)
        size = cells[dim]
        for side in (-1, 1):
            edge = 0 if side < 0 else size - 1
            c_own = lax.slice_in_dim(block, edge, edge + 1, axis=dim)
            s_own = lax.slice_in_dim(smooth, edge, edge + 1, axis=dim)
            if side > 0:
                begin = ((place[dim] + 1) * size) % whole[dim]
            else:
                begin = (place[dim] * size - 2 + whole[dim]) % whole[dim]
            begins = list(starts) + [zero]
            begins[dim] = begin.astype(jnp.int32)
            extent = [CX, CY, CZ, NORB]
            extent[dim] = 2
            slab = lax.dynamic_slice(coefficients, tuple(begins), tuple(extent))
            far_at, deep_at = (0, 1) if side > 0 else (1, 0)
            c_far = lax.slice_in_dim(slab, far_at, far_at + 1, axis=dim)
            c_deep = lax.slice_in_dim(slab, deep_at, deep_at + 1, axis=dim)
            s_far = (c_far.astype(jnp.float32) + SMOOTH * (c_deep.astype(jnp.float32) + neighbour_sum(c_far, lateral))).astype(jnp.bfloat16)
            correlation = correlation + SMOOTH * SMOOTH * gram(c_own, c_own)
            faces.append(SMOOTH * (gram(s_own, c_far) + gram(c_own, s_far)))
    scale = jnp.float32((CX * CY * CZ) ** 0.5)
    blocks = jnp.stack([correlation - jnp.eye(NORB, dtype=jnp.float32)] + faces)
    deviation = (scale * blocks).astype(jnp.bfloat16)
    product = jnp.einsum("fab,bc->fac", deviation.astype(jnp.float32), hamilton.astype(jnp.float32)).astype(jnp.bfloat16)
    return product


def reference(coefficients, potential, owner_map):
    devices = N_GX * N_GY * N_GZ

    def for_device(index):
        return one_device(index, coefficients, potential)

    products = lax.map(for_device, jnp.arange(devices, dtype=jnp.int32))
    products = products.reshape(N_GX, N_GY, N_GZ, BLOCKS, NORB, NORB)
    routes = owner_map.reshape(N_GX, N_GY, N_GZ, BLOCKS)
    order = jnp.arange(BLOCKS, dtype=jnp.int32)
    same = routes[..., :, None] == routes[..., None, :]
    earlier = order[None, :] < order[:, None]
    rank = jnp.sum((same & earlier).astype(jnp.int32), axis=-1)
    slots = jnp.arange(CAP, dtype=jnp.int32)

    def for_owner(owner):
        pick = ((routes[..., None, :] == owner) & (rank[..., None, :] == slots[:, None])).astype(jnp.float32)
        placed = jnp.einsum("xyzsf,xyzfab->yzxsab", pick, products.astype(jnp.float32), precision=lax.Precision.HIGHEST)
        return placed.reshape(N_GY, N_GZ, N_GX * CAP, NORB, NORB).astype(jnp.bfloat16)

    return lax.map(for_owner, jnp.arange(N_GX, dtype=jnp.int32))
```

```python
import functools
import math

import jax
import jax.numpy as jnp
from jax import lax
from jax.experimental import pallas as pl
from jax.experimental.pallas import tpu as pltpu
from jax.sharding import PartitionSpec as P


CAP = 2
SMOOTH = 0.25
F32 = jnp.float32
BF16 = jnp.bfloat16


def halo(low, high, axis):
    count = lax.axis_size(axis)
    up = [(i, (i + 1) % count) for i in range(count)]
    down = [((i + 1) % count, i) for i in range(count)]
    if count == 2:
        both = lax.ppermute(jnp.concatenate([high, low], axis=0), axis, up)
        return both[: high.shape[0]], both[high.shape[0] :]
    from_low = lax.ppermute(high, axis, up)
    return from_low, lax.ppermute(low, axis, down)


def local_kernel(cells, owners, c_ref, v_ref, route_ref, me_ref, lt_ref, dev_ref, ham_ref, slot_ref, c32, s32, sb, lz, lc):
    cx, cy, cz = cells
    plane = cy * cz
    width = c_ref.shape[1]
    rows = lax.broadcasted_iota(jnp.int32, (plane, plane), 0)
    cols = lax.broadcasted_iota(jnp.int32, (plane, plane), 1)
    gap = jnp.abs(rows - cols)
    beside = (gap == cz) | ((gap == 1) & ((rows // cz) == (cols // cz)))
    lateral = jnp.where(gap == 0, 1.0, jnp.where(beside, SMOOTH, 0.0)).astype(BF16)

    for x in range(cx):
        here = c_ref[x * plane : (x + 1) * plane, :]
        c32[x * plane : (x + 1) * plane, :] = here.astype(F32)
    for x in range(cx):
        at = slice(x * plane, (x + 1) * plane)
        total = jnp.dot(lateral, c_ref[at, :], preferred_element_type=F32)
        beyond = [c32[(x + d) * plane : (x + d + 1) * plane, :] for d in (-1, 1) if 0 <= x + d < cx]
        for other in beyond:
            total = total + SMOOTH * other
        s32[at, :] = total
        sb[at, :] = total.astype(BF16)

    lc[...] = jnp.zeros_like(lc)
    offset = 0
    for side in (0, 1):
        edge, deep = (0, 1) if side == 0 else (cx - 1, cx - 2)
        p = 2.0 * s32[edge * plane : (edge + 1) * plane, :] - SMOOTH * c32[deep * plane : (deep + 1) * plane, :]
        q = SMOOTH * c32[edge * plane : (edge + 1) * plane, :]
        q = q.astype(BF16)
        p = p.astype(BF16)
        first, second = (q, p) if side == 0 else (p, q)
        lt_ref[:, offset : offset + plane] = first.T
        lt_ref[:, offset + plane : offset + 2 * plane] = second.T
        shift = offset if side == 0 else offset + plane
        lc[shift : shift + plane, :] = q
        offset += 2 * plane
    for side in (0, 1):
        edge, deep = (0, 1) if side == 0 else (cy - 1, cy - 2)
        pieces = []
        for x in range(cx):
            a = x * plane + edge * cz
            b = x * plane + deep * cz
            p = (2.0 * s32[a : a + cz, :] - SMOOTH * c32[b : b + cz, :]).astype(BF16)
            q = (SMOOTH * c32[a : a + cz, :]).astype(BF16)
            pieces += [q, p] if side == 0 else [p, q]
            shift = offset + 2 * x * cz + (0 if side == 0 else cz)
            lc[shift : shift + cz, :] = q
        stacked = jnp.concatenate(pieces, axis=0)
        lt_ref[:, offset : offset + 2 * cx * cz] = stacked.T
        offset += 2 * cx * cz
    area = cx * cy
    for side in (0, 1):
        edge, deep = (0, 1) if side == 0 else (cz - 1, cz - 2)
        q = SMOOTH * c32[pl.ds(edge, area, stride=cz), :]
        p = 2.0 * s32[pl.ds(edge, area, stride=cz), :] - SMOOTH * c32[pl.ds(deep, area, stride=cz), :]
        lz[pl.ds(0 if side == 0 else 1, area, stride=2), :] = q
        lz[pl.ds(1 if side == 0 else 0, area, stride=2), :] = jnp.zeros_like(q)
        lc[offset : offset + 2 * area, :] = lz[...].astype(BF16)
        lz[pl.ds(1 if side == 0 else 0, area, stride=2), :] = p
        lt_ref[:, offset : offset + 2 * area] = lz[...].astype(BF16).T
        offset += 2 * area

    gram = jnp.dot(lt_ref[...], lc[...], preferred_element_type=F32)
    ham = jnp.zeros((width, width), F32)
    for x in range(cx):
        at = slice(x * plane, (x + 1) * plane)
        turned = sb[at, :].T
        weighted = (turned.astype(F32) * v_ref[:, at]).astype(BF16)
        both = jnp.dot(jnp.concatenate([turned, weighted], axis=0), sb[at, :], preferred_element_type=F32)
        gram = gram + both[:width]
        ham = ham + both[width:]
    ham_ref[...] = ham.astype(BF16)
    eye = (lax.broadcasted_iota(jnp.int32, (width, width), 0) == lax.broadcasted_iota(jnp.int32, (width, width), 1)).astype(F32)
    scale = math.sqrt(cx * cy * cz)
    dev_ref[...] = (scale * (gram - eye)).astype(BF16)

    count = slot_ref.shape[0]
    me = me_ref[0]
    for b in range(count):
        rank = jnp.int32(0)
        for a in range(b):
            rank = rank + (route_ref[a] == route_ref[b]).astype(jnp.int32)
        ahead = lax.rem(route_ref[b] - me + owners, owners)
        slot_ref[b, :, :] = jnp.full(slot_ref.shape[1:], ahead * CAP + rank, jnp.int32)


def place(slot_ref, b, slot, block, old):
    return jnp.where(slot_ref[b, :1, :] == slot, block, old)


def early_kernel(scale, offsets, slots, lt_ref, dev_ref, ham_ref, slot_ref, yl, yh, zl, zh, out_ref):
    ham = ham_ref[...]
    blocks = [dev_ref[...]]
    for offset, far in zip(offsets, (yl, yh, zl, zh)):
        face = jnp.dot(lt_ref[:, offset : offset + far.shape[0]], far[...], preferred_element_type=F32)
        blocks.append((scale * face).astype(BF16))
    width = ham.shape[0]
    product = jnp.dot(jnp.concatenate(blocks, axis=0), ham, preferred_element_type=F32)
    for slot in range(slots):
        total = jnp.zeros((width, width), F32)
        for i, b in enumerate((0, 3, 4, 5, 6)):
            total = place(slot_ref, b, slot, product[i * width : (i + 1) * width], total)
        out_ref[slot, :, :] = total.astype(BF16)


def late_kernel(scale, lt_ref, ham_ref, slot_ref, xl, xh, early_ref, out_ref):
    ham = ham_ref[...]
    width = ham.shape[0]
    blocks = []
    offset = 0
    for far in (xl, xh):
        face = jnp.dot(lt_ref[:, offset : offset + far.shape[0]], far[...], preferred_element_type=F32)
        blocks.append((scale * face).astype(BF16))
        offset += far.shape[0]
    product = jnp.dot(jnp.concatenate(blocks, axis=0), ham, preferred_element_type=F32)
    for slot in range(out_ref.shape[0]):
        total = early_ref[slot, :, :].astype(F32)
        for i, b in enumerate((1, 2)):
            total = place(slot_ref, b, slot, product[i * width : (i + 1) * width], total)
        out_ref[slot, :, :] = total.astype(BF16)


def local(coefficients, potential, owner_map):
    cells = coefficients.shape[:3]
    cx, cy, cz = cells
    width = coefficients.shape[3]
    blocks = owner_map.shape[3]
    owners = lax.axis_size("gx")
    me = lax.axis_index("gx")
    slots = owners * CAP
    total = cx * cy * cz
    flat = lambda layers: layers.reshape(-1, width)

    x_low, x_high = halo(flat(coefficients[:2]), flat(coefficients[cx - 2 :]), "gx")
    y_low, y_high = halo(flat(coefficients[:, :2]), flat(coefficients[:, cy - 2 :]), "gy")
    z_low, z_high = halo(flat(coefficients[:, :, :2]), flat(coefficients[:, :, cz - 2 :]), "gz")

    vmem = pl.BlockSpec(memory_space=pltpu.VMEM)
    smem = pl.BlockSpec(memory_space=pltpu.SMEM)
    factors = 4 * (cy * cz + cx * cz + cx * cy)
    sds = jax.ShapeDtypeStruct
    lt, dev, ham, slot = pl.pallas_call(
        functools.partial(local_kernel, cells, owners),
        name="own_cells",
        out_shape=(
            sds((width, factors), BF16),
            sds((width, width), BF16),
            sds((width, width), BF16),
            sds((blocks, 8, width), jnp.int32),
        ),
        in_specs=[vmem, vmem, smem, smem],
        out_specs=[vmem] * 4,
        scratch_shapes=[
            pltpu.VMEM((total, width), F32),
            pltpu.VMEM((total, width), F32),
            pltpu.VMEM((total, width), BF16),
            pltpu.VMEM((2 * cx * cy, width), F32),
            pltpu.VMEM((factors, width), BF16),
        ],
        compiler_params=pltpu.CompilerParams(vmem_limit_bytes=16 << 20),
        cost_estimate=pl.CostEstimate(flops=2_000_000_000, bytes_accessed=2 * total * width, transcendentals=0),
    )(flat(coefficients), potential.reshape(1, total), owner_map.reshape(blocks), me.reshape(1))

    scale = SMOOTH * math.sqrt(total)
    at_y = 4 * cy * cz
    at_z = at_y + 4 * cx * cz
    offsets = (at_y, at_y + 2 * cx * cz, at_z, at_z + 2 * cx * cy)
    early = pl.pallas_call(
        functools.partial(early_kernel, scale, offsets, slots),
        name="lateral_faces",
        out_shape=sds((slots, width, width), BF16),
        in_specs=[vmem] * 8,
        out_specs=vmem,
        compiler_params=pltpu.CompilerParams(vmem_limit_bytes=8 << 20),
        cost_estimate=pl.CostEstimate(flops=500_000_000, bytes_accessed=total * width, transcendentals=0),
    )(lt, dev, ham, slot, y_low, y_high, z_low, z_high)
    chosen = pl.pallas_call(
        functools.partial(late_kernel, scale),
        name="first_faces",
        out_shape=sds((slots, width, width), BF16),
        in_specs=[vmem] * 6,
        out_specs=vmem,
        compiler_params=pltpu.CompilerParams(vmem_limit_bytes=8 << 20),
        cost_estimate=pl.CostEstimate(flops=500_000_000, bytes_accessed=total * width, transcendentals=0),
    )(lt, ham, slot, x_low, x_high, early)

    pieces = [chosen[:CAP]]
    for step in range(1, owners):
        route = [(i, (i + step) % owners) for i in range(owners)]
        pieces.append(lax.ppermute(chosen[step * CAP : (step + 1) * CAP], "gx", route))

    def gather_kernel(me_ref, *refs):
        ins, out_ref, sems = refs[:owners], refs[owners], refs[owners + 1]
        copies = []
        for step in range(owners):
            source = lax.rem(me_ref[0] + owners - step, owners)
            copies.append(pltpu.make_async_copy(ins[step], out_ref.at[pl.ds(source * CAP, CAP)], sems.at[step]))
        for copy in copies:
            copy.start()
        for copy in copies:
            copy.wait()

    result = pl.pallas_call(
        gather_kernel,
        name="gather_slots",
        out_shape=sds((slots, width, width), BF16),
        in_specs=[smem] + [vmem] * owners,
        out_specs=pl.BlockSpec(memory_space=pl.ANY),
        scratch_shapes=[pltpu.SemaphoreType.DMA((owners,))],
        compiler_params=pltpu.CompilerParams(vmem_limit_bytes=8 << 20),
    )(me.reshape(1), *pieces)
    return result.reshape(1, 1, 1, slots, width, width)


def solution(mesh):
    in_specs = (P("gx", "gy", "gz", None), P("gx", "gy", "gz"), P("gx", "gy", "gz", None, None))
    out_specs = P("gx", "gy", "gz", None, None, None)
    return jax.shard_map(local, mesh=mesh, in_specs=in_specs, out_specs=out_specs, check_vma=False)
```
